128 devices in a mesh: src: 8 (over x_lo, y), col: 16 (over x_hi, z, core).
Axes of the slice: x: 4 (x_hi: 2, x_lo: 2; x = x_hi * 2 + x_lo), y: 4, z: 4, core: 2. Of those that a mesh axis runs over, the one named last changes fastest.
Arguments:
- saved_tables: float32 [8, 65536, 256], P('src', 'col'), may hold values from -6 to 6
- saved_state: float32 [8, 65536], P('src', 'col'), may hold values from 0.05 to 4
- slot_table: int32 [8], replicated, may hold values from 0 to 7, each once
- row_ids: int32 [8, 2048], replicated, may hold values from 0 to 65535
- grads: float32 [8, 256, 2048], P('src', 'col'), may hold values from -6 to 6
Outputs:
- tables_out: float32 [8, 256, 65536], P('src', 'col')
- state_out: float32 [8, 65536], P('src')
The draws below stay inside these ranges and needn't reach their ends.
Inputs may be any that keep to these rules, and one draw needn't show every extreme that they name: `slot_table`: each table is in exactly one slot. `row_ids`: row ids may repeat.
All inputs are finite; a program needn't handle non-finite values.
Results may differ from the reference program's by a relative error of at most 0.00002.
Values sent between devices are 32-bit elements; how exact they have to be, the bound alone decides.
A program may use at most 192 MiB of HBM per device.

```python
import math
import jax
import jax.numpy as jnp
import numpy as np
from jax import lax

D = 256
UPD = 2048
NT = 8
ROWS = 65536


def plant(drawn, rng, smallest, top_value):
    place = [jax.random.randint(jax.random.fold_in(rng, axis), (), 0, length) for axis, length in enumerate(drawn.shape)]
    main_axis = drawn.shape.index(max(drawn.shape))
    beside = place[:main_axis] + [(place[main_axis] + 1) % drawn.shape[main_axis]] + place[main_axis + 1:]
    return drawn.at[tuple(place)].set(smallest).at[tuple(beside)].set(top_value)


def levels(own_key, shape, split, least, top_value):
    gain, own = 1.0, jax.random.fold_in(own_key, 6)
    for dim, parts in split:
        steps = jnp.exp(jax.random.uniform(jax.random.fold_in(own, dim), (parts,), jnp.float32, least / len(split), top_value / len(split)))
        gain = gain * jnp.repeat(steps, shape[dim] // parts).reshape([-1 if axis == dim else 1 for axis in range(len(shape))])
    return gain


def cumulative_ranks(number_of, lean):
    weights = [(1 << 20) // math.isqrt(standing ** lean) + 1 for standing in range(1, number_of + 1)]
    deviation = 1 + sum(weights) // (1 << 30)
    return np.cumsum(np.array([max(1, weight // deviation) for weight in weights]))


def ranked_ids(stream_key, extent, count, slope):
    grid = cumulative_ranks(count, slope)
    ticket = jax.random.randint(jax.random.fold_in(stream_key, 1), extent, 0, int(grid[count - 1]))
    grade = jnp.searchsorted(jnp.asarray(grid, jnp.int32), ticket, side="right")
    return jax.random.permutation(jax.random.fold_in(stream_key, 2), count)[grade].astype(jnp.int32)


def gaussian(stream_key, dims, scale, reach, shards=(), held_as=jnp.bfloat16):
    factor_of = levels(stream_key, dims, shards, -0.22, 0.18) if shards else 1.0
    values = jax.random.normal(stream_key, dims, jnp.float32) * scale * factor_of
    return jnp.minimum(jnp.maximum(values, -reach), reach).astype(held_as)


def setup_inputs(seed: int = 0) -> dict:
    streams_of = jax.random.split(jax.random.key(seed), 6)
    saved_tables = gaussian(streams_of[0], (NT, ROWS, D), 1.0, 6.0, ((0, 8), (1, 16)), jnp.float32)
    saved_state = jnp.clip(jnp.exp(math.log(4.0) - 4.3820266 * jax.random.uniform(streams_of[1], (NT, ROWS), jnp.float32) ** levels(streams_of[1], (NT, ROWS), ((0, 8), (1, 16)), -0.2, 0.2)), 0.05, 4.0)
    slot_table = jax.random.permutation(streams_of[2], NT).astype(jnp.int32)
    row_ids = plant(ranked_ids(streams_of[3], (NT, UPD), ROWS, 2), jax.random.fold_in(streams_of[3], 3), 0, ROWS - 1).astype(jnp.int32)
    grads = gaussian(streams_of[4], (NT, D, UPD), 1.0, 6.0, ((0, 8), (1, 16)), jnp.float32)
    return {"saved_tables": saved_tables, "saved_state": saved_state, "slot_table": slot_table, "row_ids": row_ids, "grads": grads}


learn_rate = 0.5
epsilon = 1e-08

def reference(saved_tables, saved_state, slot_table, row_ids, grads):

    def one_slot(slot):
        table = slot_table[slot]
        weights = saved_tables[slot]
        state = saved_state[slot]
        summed = jnp.zeros((ROWS, D), jnp.float32).at[row_ids[table]].add(grads[table].T)
        new_state = state + lax.optimization_barrier(jnp.sum(summed * summed, axis=1)) / D
        new_weights = weights - learn_rate * summed / (jnp.sqrt(new_state)[:, None] + epsilon)
        return (new_weights.T, new_state)
    result = lax.map(one_slot, jnp.arange(NT, dtype=jnp.int32))
    return (result[0], result[1])
```

```python
import jax
import jax.numpy as jnp
from jax import lax
from jax.experimental import pallas as pl
from jax.experimental.pallas import tpu as pltpu
from jax.sharding import Mesh
from jax.sharding import PartitionSpec as P

D = 256
ROWS = 65536
UPD = 2048
NT = 8
NC = 16
BLK = ROWS // NC
SRC = ("xl", "y")
COL = ("xh", "z", "c")
MESH = pl.DeviceIdType.MESH
f32, bf16 = jnp.float32, jnp.bfloat16

learn_rate = 0.5
epsilon = 1e-08

FIRST = [(1, 2, 0), (0, 2, 0), (0, 1, 0), (0, 3, 0)]
SECOND = [(1, 2, 1), (1, 1, 0), (0, 2, 1)]
THIRD = [(1, 3, 1), (1, 3, 0), (1, 1, 1), (1, 0, 0), (1, 0, 1), (0, 1, 1), (0, 3, 1), (0, 0, 1)]
PEERS = FIRST + SECOND + THIRD
OTHERS = [(1, 2), (0, 2), (1, 1), (1, 3), (1, 0), (0, 1), (0, 3)]
CHUNKS = 8


def kernel(tab, st, slot, ids_all, grads, out, state_out, tabv, tT, gv, rA, sB, rB, ids_t,
           hot, hot1, acc, summed, X, stf, qs, rq, rs, seml, ssem, rsem, sst, rst, sq, rq_sem, sA, rsA, sBs, rsB):
    xl, y, xh, z, c = (lax.axis_index(a) for a in SRC + COL)
    src = xl * 4 + y
    col = xh * 8 + z * 2 + c

    def peer(o):
        nxh, nz, nc = lax.rem(xh + o[0], 2), lax.rem(z + o[1], 4), lax.rem(c + o[2], 2)
        return (xl, y, nxh, nz, nc), nxh * 8 + nz * 2 + nc

    def source(o):
        nxh, nz, nc = lax.rem(xh + 2 - o[0], 2), lax.rem(z + 4 - o[1], 4), lax.rem(c + 2 - o[2], 2)
        return nxh * 8 + nz * 2 + nc

    def other(o):
        nxl, ny = lax.rem(xl + o[0], 2), lax.rem(y + o[1], 4)
        return (nxl, ny, xh, z, c), nxl * 4 + ny

    rows = BLK // CHUNKS
    loads = []
    gl = pltpu.make_async_copy(grads.at[0], gv, seml.at[CHUNKS])
    gl.start()
    sl = pltpu.make_async_copy(st, stf.at[pl.ds(pl.multiple_of(col * 32, 32), 32)], seml.at[CHUNKS + 1])
    sl.start()
    for i in range(CHUNKS):
        cp = pltpu.make_async_copy(tab.at[0, pl.ds(i * rows, rows)], tabv.at[pl.ds(i * rows, rows)], seml.at[i])
        cp.start()
        loads.append(cp)

    barrier = pltpu.get_barrier_semaphore()
    for o in PEERS:
        pl.semaphore_signal(barrier, inc=1, device_id=peer(o)[0], device_id_type=MESH)
    for o in OTHERS:
        pl.semaphore_signal(barrier, inc=1, device_id=other(o)[0], device_id_type=MESH)

    for i in range(CHUNKS):
        loads[i].wait()
        for h in range(2):
            part = tabv[pl.ds(i * rows, rows), pl.ds(h * 128, 128)]
            tT[pl.ds(h * 8, 8), :, pl.ds(i * rows, rows)] = part.T.reshape(8, 16, rows)
    gl.wait()
    sl.wait()
    pl.semaphore_wait(barrier, len(PEERS) + len(OTHERS))

    sends_a = []
    for i, o in enumerate(OTHERS):
        device, k = other(o)
        cp = pltpu.make_async_remote_copy(
            src_ref=gv.at[:, pl.ds(pl.multiple_of(k * 256, 256), 256)], dst_ref=rA.at[src],
            send_sem=sA.at[i], recv_sem=rsA.at[i], device_id=device, device_id_type=MESH)
        cp.start()
        sends_a.append(cp)
    sends_s, sends_t = [], {}
    for i, o in enumerate(PEERS):
        own = stf.at[pl.ds(pl.multiple_of(col * 32, 32), 32)]
        cp = pltpu.make_async_remote_copy(
            src_ref=own, dst_ref=own, send_sem=sst.at[i], recv_sem=rst.at[i],
            device_id=peer(o)[0], device_id_type=MESH)
        cp.start()
        sends_s.append(cp)

    def send_tables(group):
        for o in group:
            i = PEERS.index(o)
            device, k = peer(o)
            cp = pltpu.make_async_remote_copy(
                src_ref=tT.at[k], dst_ref=out.at[0, :, pl.ds(pl.multiple_of(col * BLK, BLK), BLK)],
                send_sem=ssem.at[i], recv_sem=rsem.at[i], device_id=device, device_id_type=MESH)
            cp.start()
            sends_t[o] = cp

    send_tables(FIRST)
    rA[src] = gv[:, pl.ds(pl.multiple_of(src * 256, 256), 256)]

    ids = ids_all[pl.ds(slot[src], 1), :]
    for i in range(16):
        tile = jnp.broadcast_to(ids[:, i * 128:(i + 1) * 128], (128, 128))
        ids_t[pl.ds(i * 128, 128), :] = tile.T
    lane = lax.broadcasted_iota(jnp.int32, (256, 128), 1)
    for i in range(8):
        at = jnp.bitwise_and(ids_t[pl.ds(i * 256, 256), :], 255)
        low = (at == lane).astype(f32)
        high = (at == lane + 128).astype(f32)
        hot[pl.ds(i * 256, 256), pl.ds(0, 128)] = low.astype(bf16)
        hot[pl.ds(i * 256, 256), pl.ds(128, 128)] = high.astype(bf16)
        hot1[pl.ds(i * 256, 256), :] = (low + high).astype(bf16)

    for cp in sends_a:
        cp.wait()
    sends_b = []
    for i, o in enumerate(OTHERS):
        device, k = other(o)
        sB[i] = rA[slot[k]]
    for i, o in enumerate(OTHERS):
        device, k = other(o)
        cp = pltpu.make_async_remote_copy(
            src_ref=sB.at[i], dst_ref=rB.at[src], send_sem=sBs.at[i], recv_sem=rsB.at[i],
            device_id=device, device_id_type=MESH)
        cp.start()
        sends_b.append(cp)
    send_tables(SECOND)
    rB[src] = rA[slot[src]]
    for cp in sends_b:
        cp.wait()

    def parts(v):
        a = v.astype(bf16)
        v = v - a.astype(f32)
        b = v.astype(bf16)
        v = v - b.astype(f32)
        return a, b, v.astype(bf16)

    g = [parts(rB[p]) for p in range(8)]
    g = [jnp.concatenate([g[p][k] for p in range(8)], axis=1) for k in range(3)]
    lhs = jnp.concatenate(g + [jnp.ones((16, UPD), bf16)], axis=0)

    for i in range(8):
        row = ids_t[pl.ds(i * 256, 256), :]
        same = jnp.concatenate(
            [(row == ids[:, k * 128:(k + 1) * 128]).astype(f32).astype(bf16) for k in range(16)], axis=1)
        part = jnp.dot(lhs[:, i * 256:(i + 1) * 256], same, preferred_element_type=f32)
        if i == 0:
            acc[...] = part
        else:
            acc[...] += part
    s = acc[0:16, :] + acc[16:32, :] + acc[32:48, :]
    count = acc[48:49, :]
    q = jnp.sum(s * s, axis=0, keepdims=True)
    qs[...] = q
    rq[col] = q
    sends_q = []
    for i, o in enumerate(PEERS):
        cp = pltpu.make_async_remote_copy(
            src_ref=qs, dst_ref=rq.at[col], send_sem=sq.at[i], recv_sem=rq_sem.at[i],
            device_id=peer(o)[0], device_id_type=MESH)
        cp.start()
        sends_q.append(cp)
    send_tables(THIRD)

    high = jnp.broadcast_to(lax.shift_right_logical(ids, 8).astype(f32).astype(bf16), (16, UPD))
    zero = jnp.zeros((16, UPD), bf16)

    def dense(it, _):
        for r in range(16):
            want = (it * 16 + r).astype(f32).astype(bf16)
            mask = high == want
            for k in range(3):
                X[pl.ds(k * 256 + r * 16, 16), :] = jnp.where(mask, g[k], zero)
        o = jnp.dot(X[...], hot[...], preferred_element_type=f32)
        o = o[0:256] + o[256:512] + o[512:768]
        for r in range(16):
            summed[:, pl.ds(pl.multiple_of((it * 16 + r) * 256, 256), 256)] = o[r * 16:(r + 1) * 16]
        return 0

    lax.fori_loop(0, 16, dense, 0)

    for cp in sends_s:
        cp.wait()
    for cp in sends_q:
        cp.wait()
    total = rq[0]
    for k in range(1, NC):
        total = total + rq[k]
    tp = [jnp.broadcast_to(t, (16, UPD)) for t in parts(total / count)]
    low = lax.shift_right_logical(ids, 7)
    for b in range(4):
        for r in range(8):
            row = lax.broadcasted_iota(jnp.int32, (16, UPD), 0) + (b * 128 + r * 16)
            mask = (row == jnp.broadcast_to(low, (16, UPD))).astype(f32).astype(bf16)
            for k in range(3):
                X[pl.ds(k * 128 + r * 16, 16), :] = mask * tp[k]
        o = jnp.dot(X[pl.ds(0, 384), :], hot1[...], preferred_element_type=f32)
        new = stf[pl.ds(b * 128, 128), :] + (o[0:128] + o[128:256] + o[256:384]) / D
        state_out[pl.ds(b * 128, 128), :] = new
        rs[pl.ds(b * 128, 128), :] = learn_rate / (jnp.sqrt(new) + epsilon)

    def update(k, landed):
        def tile(t, _):
            at = pl.multiple_of(k * BLK + t * 128, 128)
            scale = jnp.broadcast_to(rs[pl.ds(k * 32 + t, 1), :], (16, 128))
            v = out[0, :, pl.ds(at, 128)] if landed else tT[k, :, pl.ds(pl.multiple_of(t * 128, 128), 128)]
            out[0, :, pl.ds(at, 128)] = v - summed[:, pl.ds(at, 128)] * scale
            return 0
        lax.fori_loop(0, 32, tile, 0, unroll=8)

    update(col, False)
    for o in PEERS:
        sends_t[o].wait()
        update(source(o), True)


def body(saved_tables, saved_state, slot_table, row_ids, grads):
    n, m = len(PEERS), len(OTHERS)
    dma = pltpu.SemaphoreType.DMA
    vmem = pl.BlockSpec(memory_space=pltpu.VMEM)
    hbm = pl.BlockSpec(memory_space=pl.ANY)
    tables, state = pl.pallas_call(
        kernel,
        out_shape=(pltpu.VMEM((1, 16, ROWS), f32), pltpu.VMEM((512, 128), f32)),
        in_specs=[hbm, hbm, pl.BlockSpec(memory_space=pltpu.SMEM), vmem, hbm],
        out_specs=(vmem, vmem),
        scratch_shapes=[
            pltpu.VMEM((BLK, D), f32), pltpu.VMEM((NC, 16, BLK), f32), pltpu.VMEM((16, UPD), f32),
            pltpu.VMEM((8, 16, 256), f32), pltpu.VMEM((7, 16, 256), f32), pltpu.VMEM((8, 16, 256), f32),
            pltpu.VMEM((UPD, 128), jnp.int32), pltpu.VMEM((UPD, 256), bf16), pltpu.VMEM((UPD, 128), bf16),
            pltpu.VMEM((64, UPD), f32), pltpu.VMEM((16, ROWS), f32), pltpu.VMEM((768, UPD), bf16),
            pltpu.VMEM((512, 128), f32), pltpu.VMEM((1, UPD), f32), pltpu.VMEM((NC, 1, UPD), f32),
            pltpu.VMEM((512, 128), f32), dma((CHUNKS + 2,)), dma((n,)), dma((n,)), dma((n,)), dma((n,)),
            dma((n,)), dma((n,)), dma((m,)), dma((m,)), dma((m,)), dma((m,)),
        ],
        compiler_params=pltpu.CompilerParams(
            collective_id=0, has_side_effects=True, vmem_limit_bytes=48 << 20),
        name="restore",
    )(saved_tables, saved_state.reshape(32, 128), slot_table, row_ids, grads)
    return (tables, state.reshape(1, ROWS))


def solution(mesh):
    split = Mesh(mesh.devices.reshape(2, 4, 2, 4, 2), SRC + COL)
    in_specs = (P(SRC, COL, None), P(SRC, COL), P(), P(), P(SRC, COL, None))
    out_specs = (P(SRC, COL, None), P(SRC, None))
    return jax.shard_map(body, mesh=split, in_specs=in_specs, out_specs=out_specs, check_vma=False)
```

```python
import jax
import jax.numpy as jnp
from jax import lax
from jax.experimental import pallas as pl
from jax.experimental.pallas import tpu as pltpu
from jax.sharding import Mesh
from jax.sharding import PartitionSpec as P

D = 256
ROWS = 65536
UPD = 2048
NT = 8
NC = 16
BLK = ROWS // NC
SRC = ("xl", "y")
COL = ("xh", "z", "c")
MESH = pl.DeviceIdType.MESH
f32, bf16 = jnp.float32, jnp.bfloat16

learn_rate = 0.5
epsilon = 1e-08

FIRST_X = [(1, 2, 0)]
FIRST_Z = [(0, 2, 0), (0, 1, 0), (0, 3, 0)]
SECOND = [(1, 2, 1), (1, 1, 0), (1, 3, 1)]
THIRD = [(0, 2, 1), (1, 0, 0), (1, 3, 0), (0, 1, 1), (0, 3, 1), (1, 1, 1), (1, 0, 1), (0, 0, 1)]
PEERS = FIRST_X + FIRST_Z + SECOND + THIRD
EARLY = FIRST_X + FIRST_Z + [(0, 0, 1)] + SECOND + [(0, 2, 1), (0, 1, 1), (0, 3, 1)]
LATE = [(1, 0, 0), (1, 3, 0), (1, 1, 1), (1, 0, 1)]
CHIPS = [(1, 2), (0, 2), (1, 1), (1, 3), (1, 0), (0, 1), (0, 3)]
OTHERS = [(1, 2), (0, 2), (1, 1), (1, 3), (1, 0), (0, 1), (0, 3)]
CHUNKS = 4


def source(o):
    xh, z, c = (lax.axis_index(a) for a in COL)
    xh, z, c = lax.rem(xh + 2 - o[0], 2), lax.rem(z + 4 - o[1], 4), lax.rem(c + 2 - o[2], 2)
    return xh * 8 + z * 2 + c


def update(k, out, summed, rs, read):
    def tile(t, _):
        at = pl.multiple_of(k * BLK + t * 128, 128)
        scale = jnp.broadcast_to(rs[pl.ds(k * 32 + t, 1), :], (16, 128))
        out[0, :, pl.ds(at, 128)] = read(at, t) - summed[:, pl.ds(at, 128)] * scale
        return 0
    lax.fori_loop(0, 32, tile, 0, unroll=8)


def kernel(tab, st, slot_h, ids_h, grads, out, state_out, summed, rs, slot, ids_all, tabv, tT, gv, rA, sB, rB,
           ids_t, hot, hot1, same, acc, X, stf, qs, qp, qh, rq, tot, seml, ssem, rsem, sst, rst, sq, rq_sem,
           sA, rsA, sBs, rsB):
    xl, y, xh, z, c = (lax.axis_index(a) for a in SRC + COL)
    src = xl * 4 + y
    col = xh * 8 + z * 2 + c

    def remote(a, b, sems, i, device):
        cp = pltpu.make_async_remote_copy(
            src_ref=a, dst_ref=b, send_sem=sems[0].at[i], recv_sem=sems[1].at[i],
            device_id=device, device_id_type=MESH)
        cp.start()
        return cp

    def peer(o):
        return (xl, y, lax.rem(xh + o[0], 2), lax.rem(z + o[1], 4), lax.rem(c + o[2], 2))

    def other(o):
        nxl, ny = lax.rem(xl + o[0], 2), lax.rem(y + o[1], 4)
        return (nxl, ny, xh, z, c), nxl * 4 + ny

    partner = peer((0, 0, 1))

    rows = BLK // CHUNKS
    first = pl.multiple_of((1 - xh) * 128, 128)
    second = pl.multiple_of(xh * 128, 128)
    small = []
    for i, (a, b) in enumerate([(grads.at[0], gv), (slot_h, slot), (ids_h, ids_all), (st, stf.at[xh, z, c])]):
        cp = pltpu.make_async_copy(a, b, seml.at[i])
        cp.start()
        small.append(cp)
    loads = []
    for h, lanes in enumerate((first, second)):
        for i in range(CHUNKS):
            cp = pltpu.make_async_copy(
                tab.at[0, pl.ds(i * rows, rows), pl.ds(lanes, 128)], tabv.at[h, pl.ds(i * rows, rows)],
                seml.at[4 + h * CHUNKS + i])
            cp.start()
            loads.append(cp)

    barrier = pltpu.get_barrier_semaphore()
    for o in PEERS:
        pl.semaphore_signal(barrier, inc=1, device_id=peer(o), device_id_type=MESH)
    for o in OTHERS:
        pl.semaphore_signal(barrier, inc=1, device_id=other(o)[0], device_id_type=MESH)

    def columns(h):
        for i in range(CHUNKS):
            loads[h * CHUNKS + i].wait()
            part = tabv[h, pl.ds(i * rows, rows), :]
            tT[h, :, :, pl.ds(i * rows, rows)] = part.T.reshape(8, 16, rows)

    sends_t = {}

    def send_tables(group):
        for o in group:
            nz, nc = lax.rem(z + o[1], 4), lax.rem(c + o[2], 2)
            sends_t[o] = remote(
                tT.at[1 - o[0], nz * 2 + nc], out.at[0, :, pl.ds(pl.multiple_of(col * BLK, BLK), BLK)],
                (ssem, rsem), PEERS.index(o), peer(o))

    columns(0)
    for cp in small:
        cp.wait()
    pl.semaphore_wait(barrier, len(PEERS) + len(OTHERS))

    sends_a = []
    for i, o in enumerate(OTHERS):
        device, k = other(o)
        sends_a.append(remote(gv.at[:, pl.ds(pl.multiple_of(k * 256, 256), 256)], rA.at[src], (sA, rsA), i, device))
    state_x = remote(stf.at[xh, z, c], stf.at[xh, z, c], (sst, rst), 0, peer((1, 0, 0)))
    send_tables(FIRST_X)
    columns(1)
    send_tables(FIRST_Z)
    rA[src] = gv[:, pl.ds(pl.multiple_of(src * 256, 256), 256)]

    ids = ids_all[pl.ds(slot[src], 1), :]
    for i in range(16):
        tile = jnp.broadcast_to(ids[:, i * 128:(i + 1) * 128], (128, 128))
        ids_t[pl.ds(i * 128, 128), :] = tile.T

    for cp in sends_a:
        cp.wait_recv()
    for i, o in enumerate(OTHERS):
        sB[i] = rA[slot[other(o)[1]]]
    rB[src] = rA[slot[src]]
    state_x.wait_recv()
    state_z = [remote(stf.at[:, z, c], stf.at[:, z, c], (sst, rst), i, peer((0, i, 0))) for i in (1, 2, 3)]
    sends_b = []
    for i, o in enumerate(OTHERS):
        sends_b.append(remote(sB.at[i], rB.at[src], (sBs, rsB), i, other(o)[0]))
    send_tables(SECOND)

    lane = lax.broadcasted_iota(jnp.int32, (256, 128), 1)
    for i in range(8):
        at = jnp.bitwise_and(ids_t[pl.ds(i * 256, 256), :], 255)
        low = (at == lane).astype(f32)
        high = (at == lane + 128).astype(f32)
        hot[pl.ds(i * 256, 256), pl.ds(0, 128)] = low.astype(bf16)
        hot[pl.ds(i * 256, 256), pl.ds(128, 128)] = high.astype(bf16)
        hot1[pl.ds(i * 256, 256), :] = (low + high).astype(bf16)
    for i in range(8):
        row = ids_t[pl.ds(i * 256, 256), :]
        for k in range(16):
            same[pl.ds(i * 256, 256), pl.ds(k * 128, 128)] = (
                row == ids[:, k * 128:(k + 1) * 128]).astype(f32).astype(bf16)

    def parts(v):
        a = v.astype(bf16)
        v = v - a.astype(f32)
        b = v.astype(bf16)
        v = v - b.astype(f32)
        return a, b, v.astype(bf16)

    for cp in sends_b:
        cp.wait_recv()
    g = [parts(rB[p]) for p in range(8)]
    g = [jnp.concatenate([g[p][k] for p in range(8)], axis=1) for k in range(3)]
    lhs = jnp.concatenate(g + [jnp.ones((16, UPD), bf16)], axis=0)

    for i in range(8):
        part = jnp.dot(lhs[:, i * 256:(i + 1) * 256], same[pl.ds(i * 256, 256), :], preferred_element_type=f32)
        if i == 0:
            acc[...] = part
        else:
            acc[...] += part
    s = acc[0:16, :] + acc[16:32, :] + acc[32:48, :]
    q = jnp.sum(s * s, axis=0, keepdims=True)
    qs[0] = q[:, :1024]
    qs[1] = q[:, 1024:]

    high = jnp.broadcast_to(lax.shift_right_logical(ids, 8).astype(f32).astype(bf16), (16, UPD))
    zero = jnp.zeros((16, UPD), bf16)

    def dense(it, _):
        for r in range(16):
            want = (it * 16 + r).astype(f32).astype(bf16)
            mask = high == want
            for k in range(3):
                X[pl.ds(k * 256 + r * 16, 16), :] = jnp.where(mask, g[k], zero)
        o = jnp.dot(X[...], hot[...], preferred_element_type=f32)
        o = o[0:256] + o[256:512] + o[512:768]
        for r in range(16):
            summed[:, pl.ds(pl.multiple_of((it * 16 + r) * 256, 256), 256)] = o[r * 16:(r + 1) * 16]
        return 0

    q_core = remote(qs.at[1 - c], qp, (sq, rq_sem), 7, partner)
    lax.fori_loop(0, 2, dense, 0)
    q_core.wait()
    half = qs[c] + qp[...]
    qh[...] = half
    rq[xh * 4 + z] = half
    lax.fori_loop(2, 3, dense, 0)
    sends_q = [remote(qh, rq.at[xh * 4 + z], (sq, rq_sem), i, peer((*o, 0))) for i, o in enumerate(CHIPS)]
    send_tables(THIRD)
    lax.fori_loop(3, 14, dense, 0)
    for cp in state_z:
        cp.wait_recv()
    state_c = remote(stf.at[:, :, c], stf.at[:, :, c], (sst, rst), 4, partner)
    for cp in sends_q:
        cp.wait_recv()
    total = rq[0]
    for k in range(1, 8):
        total = total + rq[k]
    tot[c] = total
    lax.fori_loop(14, 15, dense, 0)
    q_back = remote(tot.at[c], tot.at[c], (sq, rq_sem), 8, partner)
    lax.fori_loop(15, 16, dense, 0)
    q_back.wait_recv()
    state_c.wait_recv()

    total = jnp.concatenate([tot[0], tot[1]], axis=1) / acc[48:49, :]
    tp = [jnp.broadcast_to(t, (16, UPD)) for t in parts(total)]
    low = lax.shift_right_logical(ids, 7)
    for b in range(4):
        for r in range(8):
            row = lax.broadcasted_iota(jnp.int32, (16, UPD), 0) + (b * 128 + r * 16)
            mask = (row == jnp.broadcast_to(low, (16, UPD))).astype(f32).astype(bf16)
            for k in range(3):
                X[pl.ds(k * 128 + r * 16, 16), :] = mask * tp[k]
        o = jnp.dot(X[pl.ds(0, 384), :], hot1[...], preferred_element_type=f32)
        saved = stf[b // 2, (b % 2) * 2:(b % 2) * 2 + 2].reshape(128, 128)
        new = saved + (o[0:128] + o[128:256] + o[256:384]) / D
        state_out[pl.ds(b * 128, 128), :] = new
        rs[pl.ds(b * 128, 128), :] = learn_rate / (jnp.sqrt(new) + epsilon)

    update(col, out, summed, rs, lambda at, t: tT[1, z * 2 + c, :, pl.ds(pl.multiple_of(t * 128, 128), 128)])
    for o in EARLY:
        sends_t[o].wait_recv()
        update(source(o), out, summed, rs, lambda at, t: out[0, :, pl.ds(at, 128)])
    for o in LATE:
        sends_t[o].wait_recv()
    for cp in sends_a + sends_b + state_z + sends_q + [state_x, state_c, q_back]:
        cp.wait_send()
    for o in PEERS:
        sends_t[o].wait_send()


def finish(landed, state, summed, rs, out, state_out, sem):
    col = source((0, 0, 0))
    copies = [pltpu.make_async_copy(state, state_out, sem.at[16])]
    copies[0].start()

    def put(k):
        at = pl.ds(pl.multiple_of(k * BLK, BLK), BLK)
        cp = pltpu.make_async_copy(landed.at[0, :, at], out.at[0, :, at], sem.at[len(copies) - 1])
        cp.start()
        copies.append(cp)

    put(col)
    for o in EARLY:
        put(source(o))
    for o in LATE:
        update(source(o), landed, summed, rs, lambda at, t: landed[0, :, pl.ds(at, 128)])
        put(source(o))
    for cp in copies:
        cp.wait()


def body(saved_tables, saved_state, slot_table, row_ids, grads):
    n, m = len(PEERS), len(OTHERS)
    dma = pltpu.SemaphoreType.DMA
    vmem = pl.BlockSpec(memory_space=pltpu.VMEM)
    hbm = pl.BlockSpec(memory_space=pltpu.HBM)
    tables, state, summed, rs = pl.pallas_call(
        kernel,
        out_shape=(pltpu.VMEM((1, 16, ROWS), f32), pltpu.VMEM((512, 128), f32), pltpu.VMEM((16, ROWS), f32),
                   pltpu.VMEM((512, 128), f32)),
        in_specs=[hbm] * 5,
        out_specs=(vmem,) * 4,
        scratch_shapes=[
            pltpu.SMEM((8,), jnp.int32), pltpu.VMEM((8, UPD), jnp.int32),
            pltpu.VMEM((2, BLK, 128), f32), pltpu.VMEM((2, 8, 16, BLK), f32), pltpu.VMEM((16, UPD), f32),
            pltpu.VMEM((8, 16, 256), f32), pltpu.VMEM((7, 16, 256), f32), pltpu.VMEM((8, 16, 256), f32),
            pltpu.VMEM((UPD, 128), jnp.int32), pltpu.VMEM((UPD, 256), bf16), pltpu.VMEM((UPD, 128), bf16),
            pltpu.VMEM((UPD, UPD), bf16), pltpu.VMEM((64, UPD), f32), pltpu.VMEM((768, UPD), bf16),
            pltpu.VMEM((2, 4, 2, 32, 128), f32), pltpu.VMEM((2, 1, 1024), f32), pltpu.VMEM((1, 1024), f32),
            pltpu.VMEM((1, 1024), f32), pltpu.VMEM((8, 1, 1024), f32), pltpu.VMEM((2, 1, 1024), f32),
            dma((4 + 2 * CHUNKS,)), dma((n,)), dma((n,)), dma((5,)), dma((5,)),
            dma((9,)), dma((9,)), dma((m,)), dma((m,)), dma((m,)), dma((m,)),
        ],
        compiler_params=pltpu.CompilerParams(
            collective_id=0, has_side_effects=True, vmem_limit_bytes=44 << 20),
        name="restore",
    )(*(pltpu.with_memory_space_constraint(a, pltpu.HBM) for a in (
        saved_tables, saved_state.reshape(32, 128), slot_table, row_ids, grads)))
    tables, state = pl.pallas_call(
        finish,
        out_shape=(jax.ShapeDtypeStruct((1, 16, ROWS), f32), jax.ShapeDtypeStruct((512, 128), f32)),
        in_specs=[vmem] * 4,
        out_specs=(hbm, hbm),
        scratch_shapes=[dma((17,))],
        compiler_params=pltpu.CompilerParams(vmem_limit_bytes=16 << 20),
        name="finish",
    )(tables, state, summed, rs)
    return (tables, state.reshape(1, ROWS))


def solution(mesh):
    split = Mesh(mesh.devices.reshape(2, 4, 2, 4, 2), SRC + COL)
    in_specs = (P(SRC, COL, None), P(SRC, COL), P(), P(), P(SRC, COL, None))
    out_specs = (P(SRC, COL, None), P(SRC, None))
    return jax.shard_map(body, mesh=split, in_specs=in_specs, out_specs=out_specs, check_vma=False)
```

```python
import jax
import jax.numpy as jnp
from jax import lax
from jax.experimental import pallas as pl
from jax.experimental.pallas import tpu as pltpu
from jax.sharding import Mesh
from jax.sharding import PartitionSpec as P

D = 256
ROWS = 65536
UPD = 2048
NT = 8
NC = 16
BLK = ROWS // NC
SRC = ("xl", "y")
COL = ("xh", "z", "c")
MESH = pl.DeviceIdType.MESH
f32, bf16 = jnp.float32, jnp.bfloat16

learn_rate = 0.5
epsilon = 1e-08

FIRST_X = [(1, 1, 0)]
FIRST_Z = [(0, 1, 0), (0, 3, 0), (0, 2, 0)]
SECOND = [(1, 2, 0), (1, 3, 0), (1, 0, 0)]
THIRD = [(0, 1, 1), (1, 1, 1), (1, 2, 1), (0, 3, 1), (0, 2, 1), (1, 3, 1), (1, 0, 1), (0, 0, 1)]
PEERS = FIRST_X + FIRST_Z + SECOND + THIRD
EARLY = [(1, 1, 0), (0, 2, 0), (0, 1, 0), (0, 3, 0), (0, 0, 1), (1, 2, 0), (1, 0, 0), (1, 3, 0), (0, 2, 1), (0, 1, 1), (0, 3, 1)]
LATE = [(1, 1, 1), (1, 2, 1), (1, 3, 1), (1, 0, 1)]
CHIPS = [(1, 2), (0, 2), (1, 1), (1, 3), (1, 0), (0, 1), (0, 3)]
OTHERS = [(1, 2), (0, 2), (1, 1), (1, 3), (1, 0), (0, 1), (0, 3)]
CHUNKS = 4


def turn(o, c):
    return o[1] + 2 * c if o[0] else o[1]


def source(o):
    xh, z, c = (lax.axis_index(a) for a in COL)
    xh, c = lax.rem(xh + 2 - o[0], 2), lax.rem(c + 2 - o[2], 2)
    return xh * 8 + lax.rem(z + 8 - turn(o, c), 4) * 2 + c


def update(k, out, summed, rs, read):
    def tile(t, _):
        at = pl.multiple_of(k * BLK + t * 128, 128)
        scale = jnp.broadcast_to(rs[pl.ds(k * 32 + t, 1), :], (16, 128))
        out[0, :, pl.ds(at, 128)] = read(at, t) - summed[:, pl.ds(at, 128)] * scale
        return 0
    lax.fori_loop(0, 32, tile, 0, unroll=8)


def kernel(tab, st, slot_h, ids_h, grads, out, state_out, summed, rs, slot, ids_all, tabv, tT, gv, rA, sB, rB,
           ids_t, hot, hot1, same, acc, X, stf, qs, qp, qh, rq, tot, seml, ssem, rsem, sst, rst, sq, rq_sem,
           sA, rsA, sBs, rsB):
    xl, y, xh, z, c = (lax.axis_index(a) for a in SRC + COL)
    src = xl * 4 + y
    col = xh * 8 + z * 2 + c

    def remote(a, b, sems, i, device):
        cp = pltpu.make_async_remote_copy(
            src_ref=a, dst_ref=b, send_sem=sems[0].at[i], recv_sem=sems[1].at[i],
            device_id=device, device_id_type=MESH)
        cp.start()
        return cp

    def peer(o):
        return (xl, y, lax.rem(xh + o[0], 2), lax.rem(z + o[1], 4), lax.rem(c + o[2], 2))

    def other(o):
        nxl, ny = lax.rem(xl + o[0], 2), lax.rem(y + o[1], 4)
        return (nxl, ny, xh, z, c), nxl * 4 + ny

    partner = peer((0, 0, 1))

    barrier = pltpu.get_barrier_semaphore()
    for o in PEERS:
        pl.semaphore_signal(barrier, inc=1, device_id=peer(o), device_id_type=MESH)
    for o in OTHERS:
        pl.semaphore_signal(barrier, inc=1, device_id=other(o)[0], device_id_type=MESH)

    rows = BLK // CHUNKS
    first = pl.multiple_of((1 - xh) * 128, 128)
    second = pl.multiple_of(xh * 128, 128)
    small = []
    for i, (a, b) in enumerate([(grads.at[0], gv), (slot_h, slot), (ids_h, ids_all), (st, stf.at[xh, z, c])]):
        cp = pltpu.make_async_copy(a, b, seml.at[i])
        cp.start()
        small.append(cp)
    loads = []
    for h, lanes in enumerate((first, second)):
        for i in range(CHUNKS):
            cp = pltpu.make_async_copy(
                tab.at[0, pl.ds(i * rows, rows), pl.ds(lanes, 128)], tabv.at[h, pl.ds(i * rows, rows)],
                seml.at[4 + h * CHUNKS + i])
            cp.start()
            loads.append(cp)

    def columns(h):
        for i in range(CHUNKS):
            loads[h * CHUNKS + i].wait()
            part = tabv[h, pl.ds(i * rows, rows), :]
            tT[h, :, :, pl.ds(i * rows, rows)] = part.T.reshape(8, 16, rows)

    sends_t = {}

    def send_tables(group):
        for o in group:
            nz, nc = lax.rem(z + turn(o, c), 4), lax.rem(c + o[2], 2)
            sends_t[o] = remote(
                tT.at[1 - o[0], nz * 2 + nc], out.at[0, :, pl.ds(pl.multiple_of(col * BLK, BLK), BLK)],
                (ssem, rsem), PEERS.index(o), (xl, y, lax.rem(xh + o[0], 2), nz, nc))

    columns(0)
    for cp in small:
        cp.wait()
    pl.semaphore_wait(barrier, len(PEERS) + len(OTHERS))

    sends_a = []
    for i, o in enumerate(OTHERS):
        device, k = other(o)
        sends_a.append(remote(gv.at[:, pl.ds(pl.multiple_of(k * 256, 256), 256)], rA.at[src], (sA, rsA), i, device))
    state_x = remote(stf.at[xh, z, c], stf.at[xh, z, c], (sst, rst), 0, peer((1, 0, 0)))
    send_tables(FIRST_X)
    columns(1)
    send_tables(FIRST_Z)
    rA[src] = gv[:, pl.ds(pl.multiple_of(src * 256, 256), 256)]

    ids = ids_all[pl.ds(slot[src], 1), :]
    for i in range(16):
        tile = jnp.broadcast_to(ids[:, i * 128:(i + 1) * 128], (128, 128))
        ids_t[pl.ds(i * 128, 128), :] = tile.T

    for cp in sends_a:
        cp.wait_recv()
    for i, o in enumerate(OTHERS):
        sB[i] = rA[slot[other(o)[1]]]
    rB[src] = rA[slot[src]]
    state_x.wait_recv()
    state_z = [remote(stf.at[:, z, c], stf.at[:, z, c], (sst, rst), i, peer((0, i, 0))) for i in (1, 2, 3)]
    sends_b = []
    for i, o in enumerate(OTHERS):
        sends_b.append(remote(sB.at[i], rB.at[src], (sBs, rsB), i, other(o)[0]))
    send_tables(SECOND)

    lane = lax.broadcasted_iota(jnp.int32, (256, 128), 1)
    for i in range(8):
        at = jnp.bitwise_and(ids_t[pl.ds(i * 256, 256), :], 255)
        low = (at == lane).astype(f32)
        high = (at == lane + 128).astype(f32)
        hot[pl.ds(i * 256, 256), pl.ds(0, 128)] = low.astype(bf16)
        hot[pl.ds(i * 256, 256), pl.ds(128, 128)] = high.astype(bf16)
        hot1[pl.ds(i * 256, 256), :] = (low + high).astype(bf16)
    for i in range(8):
        row = ids_t[pl.ds(i * 256, 256), :]
        for k in range(16):
            same[pl.ds(i * 256, 256), pl.ds(k * 128, 128)] = (
                row == ids[:, k * 128:(k + 1) * 128]).astype(f32).astype(bf16)

    def parts(v):
        a = v.astype(bf16)
        v = v - a.astype(f32)
        b = v.astype(bf16)
        v = v - b.astype(f32)
        return a, b, v.astype(bf16)

    for cp in sends_b:
        cp.wait_recv()
    g = [parts(rB[p]) for p in range(8)]
    g = [jnp.concatenate([g[p][k] for p in range(8)], axis=1) for k in range(3)]
    lhs = jnp.concatenate(g + [jnp.ones((16, UPD), bf16)], axis=0)

    for i in range(8):
        part = jnp.dot(lhs[:, i * 256:(i + 1) * 256], same[pl.ds(i * 256, 256), :], preferred_element_type=f32)
        if i == 0:
            acc[...] = part
        else:
            acc[...] += part
    s = acc[0:16, :] + acc[16:32, :] + acc[32:48, :]
    q = jnp.sum(s * s, axis=0, keepdims=True)
    qs[0] = q[:, :1024]
    qs[1] = q[:, 1024:]

    high = jnp.broadcast_to(lax.shift_right_logical(ids, 8).astype(f32).astype(bf16), (16, UPD))
    zero = jnp.zeros((16, UPD), bf16)

    def dense(it, _):
        for r in range(16):
            want = (it * 16 + r).astype(f32).astype(bf16)
            mask = high == want
            for k in range(3):
                X[pl.ds(k * 256 + r * 16, 16), :] = jnp.where(mask, g[k], zero)
        o = jnp.dot(X[...], hot[...], preferred_element_type=f32)
        o = o[0:256] + o[256:512] + o[512:768]
        for r in range(16):
            summed[:, pl.ds(pl.multiple_of((it * 16 + r) * 256, 256), 256)] = o[r * 16:(r + 1) * 16]
        return 0

    q_core = remote(qs.at[1 - c], qp, (sq, rq_sem), 7, partner)
    lax.fori_loop(0, 2, dense, 0)
    q_core.wait()
    half = qs[c] + qp[...]
    qh[...] = half
    rq[xh * 4 + z] = half
    lax.fori_loop(2, 3, dense, 0)
    sends_q = [remote(qh, rq.at[xh * 4 + z], (sq, rq_sem), i, peer((*o, 0))) for i, o in enumerate(CHIPS)]
    send_tables(THIRD)
    lax.fori_loop(3, 14, dense, 0)
    for cp in state_z:
        cp.wait_recv()
    state_c = remote(stf.at[:, :, c], stf.at[:, :, c], (sst, rst), 4, partner)
    for cp in sends_q:
        cp.wait_recv()
    total = rq[0]
    for k in range(1, 8):
        total = total + rq[k]
    tot[c] = total
    lax.fori_loop(14, 15, dense, 0)
    q_back = remote(tot.at[c], tot.at[c], (sq, rq_sem), 8, partner)
    lax.fori_loop(15, 16, dense, 0)
    q_back.wait_recv()
    state_c.wait_recv()

    total = jnp.concatenate([tot[0], tot[1]], axis=1) / acc[48:49, :]
    tp = [jnp.broadcast_to(t, (16, UPD)) for t in parts(total)]
    low = lax.shift_right_logical(ids, 7)
    for b in range(4):
        for r in range(8):
            row = lax.broadcasted_iota(jnp.int32, (16, UPD), 0) + (b * 128 + r * 16)
            mask = (row == jnp.broadcast_to(low, (16, UPD))).astype(f32).astype(bf16)
            for k in range(3):
                X[pl.ds(k * 128 + r * 16, 16), :] = mask * tp[k]
        o = jnp.dot(X[pl.ds(0, 384), :], hot1[...], preferred_element_type=f32)
        saved = stf[b // 2, (b % 2) * 2:(b % 2) * 2 + 2].reshape(128, 128)
        new = saved + (o[0:128] + o[128:256] + o[256:384]) / D
        state_out[pl.ds(b * 128, 128), :] = new
        rs[pl.ds(b * 128, 128), :] = learn_rate / (jnp.sqrt(new) + epsilon)

    update(col, out, summed, rs, lambda at, t: tT[1, z * 2 + c, :, pl.ds(pl.multiple_of(t * 128, 128), 128)])
    for o in EARLY:
        sends_t[o].wait_recv()
        update(source(o), out, summed, rs, lambda at, t: out[0, :, pl.ds(at, 128)])
    for o in LATE:
        sends_t[o].wait_recv()
    for cp in sends_a + sends_b + state_z + sends_q + [state_x, state_c, q_back]:
        cp.wait_send()
    for o in PEERS:
        sends_t[o].wait_send()


def finish(landed, state, summed, rs, out, state_out, sem):
    col = source((0, 0, 0))
    copies = [pltpu.make_async_copy(state, state_out, sem.at[16])]
    copies[0].start()

    def put(k):
        at = pl.ds(pl.multiple_of(k * BLK, BLK), BLK)
        cp = pltpu.make_async_copy(landed.at[0, :, at], out.at[0, :, at], sem.at[len(copies) - 1])
        cp.start()
        copies.append(cp)

    put(col)
    for o in EARLY:
        put(source(o))
    for o in LATE:
        update(source(o), landed, summed, rs, lambda at, t: landed[0, :, pl.ds(at, 128)])
        put(source(o))
    for cp in copies:
        cp.wait()


def body(saved_tables, saved_state, slot_table, row_ids, grads):
    n, m = len(PEERS), len(OTHERS)
    dma = pltpu.SemaphoreType.DMA
    vmem = pl.BlockSpec(memory_space=pltpu.VMEM)
    hbm = pl.BlockSpec(memory_space=pltpu.HBM)
    tables, state, summed, rs = pl.pallas_call(
        kernel,
        out_shape=(pltpu.VMEM((1, 16, ROWS), f32), pltpu.VMEM((512, 128), f32), pltpu.VMEM((16, ROWS), f32),
                   pltpu.VMEM((512, 128), f32)),
        in_specs=[hbm] * 5,
        out_specs=(vmem,) * 4,
        scratch_shapes=[
            pltpu.SMEM((8,), jnp.int32), pltpu.VMEM((8, UPD), jnp.int32),
            pltpu.VMEM((2, BLK, 128), f32), pltpu.VMEM((2, 8, 16, BLK), f32), pltpu.VMEM((16, UPD), f32),
            pltpu.VMEM((8, 16, 256), f32), pltpu.VMEM((7, 16, 256), f32), pltpu.VMEM((8, 16, 256), f32),
            pltpu.VMEM((UPD, 128), jnp.int32), pltpu.VMEM((UPD, 256), bf16), pltpu.VMEM((UPD, 128), bf16),
            pltpu.VMEM((UPD, UPD), bf16), pltpu.VMEM((64, UPD), f32), pltpu.VMEM((768, UPD), bf16),
            pltpu.VMEM((2, 4, 2, 32, 128), f32), pltpu.VMEM((2, 1, 1024), f32), pltpu.VMEM((1, 1024), f32),
            pltpu.VMEM((1, 1024), f32), pltpu.VMEM((8, 1, 1024), f32), pltpu.VMEM((2, 1, 1024), f32),
            dma((4 + 2 * CHUNKS,)), dma((n,)), dma((n,)), dma((5,)), dma((5,)),
            dma((9,)), dma((9,)), dma((m,)), dma((m,)), dma((m,)), dma((m,)),
        ],
        compiler_params=pltpu.CompilerParams(
            collective_id=0, has_side_effects=True, vmem_limit_bytes=44 << 20),
        name="restore",
    )(*(pltpu.with_memory_space_constraint(a, pltpu.HBM) for a in (
        saved_tables, saved_state.reshape(32, 128), slot_table, row_ids, grads)))
    tables, state = pl.pallas_call(
        finish,
        out_shape=(jax.ShapeDtypeStruct((1, 16, ROWS), f32), jax.ShapeDtypeStruct((512, 128), f32)),
        in_specs=[vmem] * 4,
        out_specs=(hbm, hbm),
        scratch_shapes=[dma((17,))],
        compiler_params=pltpu.CompilerParams(vmem_limit_bytes=16 << 20),
        name="finish",
    )(tables, state, summed, rs)
    return (tables, state.reshape(1, ROWS))


def solution(mesh):
    split = Mesh(mesh.devices.reshape(2, 4, 2, 4, 2), SRC + COL)
    in_specs = (P(SRC, COL, None), P(SRC, COL), P(), P(), P(SRC, COL, None))
    out_specs = (P(SRC, COL, None), P(SRC, None))
    return jax.shard_map(body, mesh=split, in_specs=in_specs, out_specs=out_specs, check_vma=False)
```

```python
import jax
import jax.numpy as jnp
from jax import lax
from jax.experimental import pallas as pl
from jax.experimental.pallas import tpu as pltpu
from jax.sharding import Mesh
from jax.sharding import PartitionSpec as P

D = 256
ROWS = 65536
UPD = 2048
NT = 8
NC = 16
BLK = ROWS // NC
SRC = ("xl", "y")
COL = ("xh", "z", "c")
MESH = pl.DeviceIdType.MESH
f32, bf16 = jnp.float32, jnp.bfloat16

learn_rate = 0.5
epsilon = 1e-08

FIRST_X = [(1, 1, 0)]
FIRST_Z = [(0, 1, 0), (0, 3, 0), (0, 2, 0)]
SECOND = [(1, 2, 0), (1, 3, 0), (1, 0, 0)]
THIRD = [(0, 1, 1), (1, 1, 1), (1, 2, 1), (0, 3, 1), (0, 2, 1), (1, 3, 1), (1, 0, 1), (0, 0, 1)]
PEERS = FIRST_X + FIRST_Z + SECOND + THIRD
EARLY = [(1, 1, 0), (0, 2, 0), (0, 1, 0), (0, 3, 0), (0, 0, 1), (1, 2, 0), (1, 0, 0), (1, 3, 0), (0, 2, 1), (0, 1, 1), (0, 3, 1)]
LATE = [(1, 1, 1), (1, 2, 1), (1, 3, 1), (1, 0, 1)]
CHIPS = [(1, 2), (0, 2), (1, 1), (1, 3), (1, 0), (0, 1), (0, 3)]
OTHERS = [(1, 2), (0, 2), (1, 1), (1, 3), (1, 0), (0, 1), (0, 3)]
CHUNKS = 4


def turn(o, c):
    return o[1] + 3 * c if o[0] else o[1]


def source(o):
    xh, z, c = (lax.axis_index(a) for a in COL)
    xh, c = lax.rem(xh + 2 - o[0], 2), lax.rem(c + 2 - o[2], 2)
    return xh * 8 + lax.rem(z + 8 - turn(o, c), 4) * 2 + c


def update(k, out, summed, rs, read):
    def tile(t, _):
        at = pl.multiple_of(k * BLK + t * 128, 128)
        scale = jnp.broadcast_to(rs[pl.ds(k * 32 + t, 1), :], (16, 128))
        out[0, :, pl.ds(at, 128)] = read(at, t) - summed[:, pl.ds(at, 128)] * scale
        return 0
    lax.fori_loop(0, 32, tile, 0, unroll=8)


def kernel(tab, st, slot_h, ids_h, grads, out, state_out, summed, rs, slot, ids_all, tabv, tT, gv, rA, sB, rB,
           ids_t, hot, hot1, same, acc, X, stf, qs, qp, qh, rq, tot, seml, ssem, rsem, sst, rst, sq, rq_sem,
           sA, rsA, sBs, rsB):
    xl, y, xh, z, c = (lax.axis_index(a) for a in SRC + COL)
    src = xl * 4 + y
    col = xh * 8 + z * 2 + c

    def remote(a, b, sems, i, device):
        cp = pltpu.make_async_remote_copy(
            src_ref=a, dst_ref=b, send_sem=sems[0].at[i], recv_sem=sems[1].at[i],
            device_id=device, device_id_type=MESH)
        cp.start()
        return cp

    def peer(o):
        return (xl, y, lax.rem(xh + o[0], 2), lax.rem(z + o[1], 4), lax.rem(c + o[2], 2))

    def other(o):
        nxl, ny = lax.rem(xl + o[0], 2), lax.rem(y + o[1], 4)
        return (nxl, ny, xh, z, c), nxl * 4 + ny

    partner = peer((0, 0, 1))

    barrier = pltpu.get_barrier_semaphore()
    for o in PEERS:
        pl.semaphore_signal(barrier, inc=1, device_id=peer(o), device_id_type=MESH)
    for o in OTHERS:
        pl.semaphore_signal(barrier, inc=1, device_id=other(o)[0], device_id_type=MESH)

    rows = BLK // CHUNKS
    first = pl.multiple_of((1 - xh) * 128, 128)
    second = pl.multiple_of(xh * 128, 128)
    small = []
    for i, (a, b) in enumerate([(grads.at[0], gv), (slot_h, slot), (ids_h, ids_all), (st, stf.at[xh, z, c])]):
        cp = pltpu.make_async_copy(a, b, seml.at[i])
        cp.start()
        small.append(cp)
    loads = []
    for h, lanes in enumerate((first, second)):
        for i in range(CHUNKS):
            cp = pltpu.make_async_copy(
                tab.at[0, pl.ds(i * rows, rows), pl.ds(lanes, 128)], tabv.at[h, pl.ds(i * rows, rows)],
                seml.at[4 + h * CHUNKS + i])
            cp.start()
            loads.append(cp)

    def columns(h):
        for i in range(CHUNKS):
            loads[h * CHUNKS + i].wait()
            part = tabv[h, pl.ds(i * rows, rows), :]
            tT[h, :, :, pl.ds(i * rows, rows)] = part.T.reshape(8, 16, rows)

    sends_t = {}

    def send_tables(group):
        for o in group:
            nz, nc = lax.rem(z + turn(o, c), 4), lax.rem(c + o[2], 2)
            sends_t[o] = remote(
                tT.at[1 - o[0], nz * 2 + nc], out.at[0, :, pl.ds(pl.multiple_of(col * BLK, BLK), BLK)],
                (ssem, rsem), PEERS.index(o), (xl, y, lax.rem(xh + o[0], 2), nz, nc))

    columns(0)
    for cp in small:
        cp.wait()
    pl.semaphore_wait(barrier, len(PEERS) + len(OTHERS))

    sends_a = []
    for i, o in enumerate(OTHERS):
        device, k = other(o)
        sends_a.append(remote(gv.at[:, pl.ds(pl.multiple_of(k * 256, 256), 256)], rA.at[src], (sA, rsA), i, device))
    state_x = remote(stf.at[xh, z, c], stf.at[xh, z, c], (sst, rst), 0, peer((1, 0, 0)))
    send_tables(FIRST_X)
    columns(1)
    send_tables(FIRST_Z)
    rA[src] = gv[:, pl.ds(pl.multiple_of(src * 256, 256), 256)]

    ids = ids_all[pl.ds(slot[src], 1), :]
    for i in range(16):
        tile = jnp.broadcast_to(ids[:, i * 128:(i + 1) * 128], (128, 128))
        ids_t[pl.ds(i * 128, 128), :] = tile.T

    for cp in sends_a:
        cp.wait_recv()
    for i, o in enumerate(OTHERS):
        sB[i] = rA[slot[other(o)[1]]]
    rB[src] = rA[slot[src]]
    state_x.wait_recv()
    state_z = [remote(stf.at[:, z, c], stf.at[:, z, c], (sst, rst), i, peer((0, i, 0))) for i in (1, 2, 3)]
    sends_b = []
    for i, o in enumerate(OTHERS):
        sends_b.append(remote(sB.at[i], rB.at[src], (sBs, rsB), i, other(o)[0]))
    send_tables(SECOND)

    lane = lax.broadcasted_iota(jnp.int32, (256, 128), 1)
    for i in range(8):
        at = jnp.bitwise_and(ids_t[pl.ds(i * 256, 256), :], 255)
        low = (at == lane).astype(f32)
        high = (at == lane + 128).astype(f32)
        hot[pl.ds(i * 256, 256), pl.ds(0, 128)] = low.astype(bf16)
        hot[pl.ds(i * 256, 256), pl.ds(128, 128)] = high.astype(bf16)
        hot1[pl.ds(i * 256, 256), :] = (low + high).astype(bf16)
    for i in range(8):
        row = ids_t[pl.ds(i * 256, 256), :]
        for k in range(16):
            same[pl.ds(i * 256, 256), pl.ds(k * 128, 128)] = (
                row == ids[:, k * 128:(k + 1) * 128]).astype(f32).astype(bf16)

    def parts(v):
        a = v.astype(bf16)
        v = v - a.astype(f32)
        b = v.astype(bf16)
        v = v - b.astype(f32)
        return a, b, v.astype(bf16)

    for cp in sends_b:
        cp.wait_recv()
    g = [parts(rB[p]) for p in range(8)]
    g = [jnp.concatenate([g[p][k] for p in range(8)], axis=1) for k in range(3)]
    lhs = jnp.concatenate(g + [jnp.ones((16, UPD), bf16)], axis=0)

    for i in range(8):
        part = jnp.dot(lhs[:, i * 256:(i + 1) * 256], same[pl.ds(i * 256, 256), :], preferred_element_type=f32)
        if i == 0:
            acc[...] = part
        else:
            acc[...] += part
    s = acc[0:16, :] + acc[16:32, :] + acc[32:48, :]
    q = jnp.sum(s * s, axis=0, keepdims=True)
    qs[0] = q[:, :1024]
    qs[1] = q[:, 1024:]

    high = jnp.broadcast_to(lax.shift_right_logical(ids, 8).astype(f32).astype(bf16), (16, UPD))
    zero = jnp.zeros((16, UPD), bf16)

    def dense(it, _):
        for r in range(16):
            want = (it * 16 + r).astype(f32).astype(bf16)
            mask = high == want
            for k in range(3):
                X[pl.ds(k * 256 + r * 16, 16), :] = jnp.where(mask, g[k], zero)
        o = jnp.dot(X[...], hot[...], preferred_element_type=f32)
        o = o[0:256] + o[256:512] + o[512:768]
        for r in range(16):
            summed[:, pl.ds(pl.multiple_of((it * 16 + r) * 256, 256), 256)] = o[r * 16:(r + 1) * 16]
        return 0

    q_core = remote(qs.at[1 - c], qp, (sq, rq_sem), 7, partner)
    lax.fori_loop(0, 2, dense, 0)
    q_core.wait()
    half = qs[c] + qp[...]
    qh[...] = half
    rq[xh * 4 + z] = half
    lax.fori_loop(2, 3, dense, 0)
    sends_q = [remote(qh, rq.at[xh * 4 + z], (sq, rq_sem), i, peer((*o, 0))) for i, o in enumerate(CHIPS)]
    send_tables(THIRD)
    lax.fori_loop(3, 14, dense, 0)
    for cp in state_z:
        cp.wait_recv()
    state_c = remote(stf.at[:, :, c], stf.at[:, :, c], (sst, rst), 4, partner)
    for cp in sends_q:
        cp.wait_recv()
    total = rq[0]
    for k in range(1, 8):
        total = total + rq[k]
    tot[c] = total
    lax.fori_loop(14, 15, dense, 0)
    q_back = remote(tot.at[c], tot.at[c], (sq, rq_sem), 8, partner)
    lax.fori_loop(15, 16, dense, 0)
    q_back.wait_recv()
    state_c.wait_recv()

    total = jnp.concatenate([tot[0], tot[1]], axis=1) / acc[48:49, :]
    tp = [jnp.broadcast_to(t, (16, UPD)) for t in parts(total)]
    low = lax.shift_right_logical(ids, 7)
    for b in range(4):
        for r in range(8):
            row = lax.broadcasted_iota(jnp.int32, (16, UPD), 0) + (b * 128 + r * 16)
            mask = (row == jnp.broadcast_to(low, (16, UPD))).astype(f32).astype(bf16)
            for k in range(3):
                X[pl.ds(k * 128 + r * 16, 16), :] = mask * tp[k]
        o = jnp.dot(X[pl.ds(0, 384), :], hot1[...], preferred_element_type=f32)
        saved = stf[b // 2, (b % 2) * 2:(b % 2) * 2 + 2].reshape(128, 128)
        new = saved + (o[0:128] + o[128:256] + o[256:384]) / D
        state_out[pl.ds(b * 128, 128), :] = new
        rs[pl.ds(b * 128, 128), :] = learn_rate / (jnp.sqrt(new) + epsilon)

    update(col, out, summed, rs, lambda at, t: tT[1, z * 2 + c, :, pl.ds(pl.multiple_of(t * 128, 128), 128)])
    for o in EARLY:
        sends_t[o].wait_recv()
        update(source(o), out, summed, rs, lambda at, t: out[0, :, pl.ds(at, 128)])
    for o in LATE:
        sends_t[o].wait_recv()
    for cp in sends_a + sends_b + state_z + sends_q + [state_x, state_c, q_back]:
        cp.wait_send()
    for o in PEERS:
        sends_t[o].wait_send()


def finish(landed, state, summed, rs, out, state_out, sem):
    col = source((0, 0, 0))
    copies = [pltpu.make_async_copy(state, state_out, sem.at[16])]
    copies[0].start()

    def put(k):
        at = pl.ds(pl.multiple_of(k * BLK, BLK), BLK)
        cp = pltpu.make_async_copy(landed.at[0, :, at], out.at[0, :, at], sem.at[len(copies) - 1])
        cp.start()
        copies.append(cp)

    put(col)
    for o in EARLY:
        put(source(o))
    for o in LATE:
        update(source(o), landed, summed, rs, lambda at, t: landed[0, :, pl.ds(at, 128)])
        put(source(o))
    for cp in copies:
        cp.wait()


def body(saved_tables, saved_state, slot_table, row_ids, grads):
    n, m = len(PEERS), len(OTHERS)
    dma = pltpu.SemaphoreType.DMA
    vmem = pl.BlockSpec(memory_space=pltpu.VMEM)
    hbm = pl.BlockSpec(memory_space=pltpu.HBM)
    tables, state, summed, rs = pl.pallas_call(
        kernel,
        out_shape=(pltpu.VMEM((1, 16, ROWS), f32), pltpu.VMEM((512, 128), f32), pltpu.VMEM((16, ROWS), f32),
                   pltpu.VMEM((512, 128), f32)),
        in_specs=[hbm] * 5,
        out_specs=(vmem,) * 4,
        scratch_shapes=[
            pltpu.SMEM((8,), jnp.int32), pltpu.VMEM((8, UPD), jnp.int32),
            pltpu.VMEM((2, BLK, 128), f32), pltpu.VMEM((2, 8, 16, BLK), f32), pltpu.VMEM((16, UPD), f32),
            pltpu.VMEM((8, 16, 256), f32), pltpu.VMEM((7, 16, 256), f32), pltpu.VMEM((8, 16, 256), f32),
            pltpu.VMEM((UPD, 128), jnp.int32), pltpu.VMEM((UPD, 256), bf16), pltpu.VMEM((UPD, 128), bf16),
            pltpu.VMEM((UPD, UPD), bf16), pltpu.VMEM((64, UPD), f32), pltpu.VMEM((768, UPD), bf16),
            pltpu.VMEM((2, 4, 2, 32, 128), f32), pltpu.VMEM((2, 1, 1024), f32), pltpu.VMEM((1, 1024), f32),
            pltpu.VMEM((1, 1024), f32), pltpu.VMEM((8, 1, 1024), f32), pltpu.VMEM((2, 1, 1024), f32),
            dma((4 + 2 * CHUNKS,)), dma((n,)), dma((n,)), dma((5,)), dma((5,)),
            dma((9,)), dma((9,)), dma((m,)), dma((m,)), dma((m,)), dma((m,)),
        ],
        compiler_params=pltpu.CompilerParams(
            collective_id=0, has_side_effects=True, vmem_limit_bytes=44 << 20),
        name="restore",
    )(*(pltpu.with_memory_space_constraint(a, pltpu.HBM) for a in (
        saved_tables, saved_state.reshape(32, 128), slot_table, row_ids, grads)))
    tables, state = pl.pallas_call(
        finish,
        out_shape=(jax.ShapeDtypeStruct((1, 16, ROWS), f32), jax.ShapeDtypeStruct((512, 128), f32)),
        in_specs=[vmem] * 4,
        out_specs=(hbm, hbm),
        scratch_shapes=[dma((17,))],
        compiler_params=pltpu.CompilerParams(vmem_limit_bytes=16 << 20),
        name="finish",
    )(tables, state, summed, rs)
    return (tables, state.reshape(1, ROWS))


def solution(mesh):
    split = Mesh(mesh.devices.reshape(2, 4, 2, 4, 2), SRC + COL)
    in_specs = (P(SRC, COL, None), P(SRC, COL), P(), P(), P(SRC, COL, None))
    out_specs = (P(SRC, COL, None), P(SRC, None))
    return jax.shard_map(body, mesh=split, in_specs=in_specs, out_specs=out_specs, check_vma=False)
```

```python
import jax
import jax.numpy as jnp
from jax import lax
from jax.experimental import pallas as pl
from jax.experimental.pallas import tpu as pltpu
from jax.sharding import Mesh
from jax.sharding import PartitionSpec as P

D = 256
ROWS = 65536
UPD = 2048
NT = 8
NC = 16
BLK = ROWS // NC
SRC = ("xl", "y")
COL = ("xh", "z", "c")
MESH = pl.DeviceIdType.MESH
f32, bf16 = jnp.float32, jnp.bfloat16

learn_rate = 0.5
epsilon = 1e-08

FIRST_X = [(1, 1, 0)]
FIRST_Z = [(0, 1, 0), (0, 3, 0), (0, 2, 0)]
SECOND = [(1, 2, 0), (1, 3, 0), (1, 0, 0)]
THIRD = [(0, 1, 1), (1, 1, 1), (1, 2, 1), (0, 3, 1), (0, 2, 1), (1, 3, 1), (1, 0, 1), (0, 0, 1)]
PEERS = FIRST_X + FIRST_Z + SECOND + THIRD
EARLY = [(1, 1, 0), (0, 2, 0), (0, 1, 0), (0, 3, 0), (0, 0, 1), (1, 2, 0), (1, 0, 0), (1, 3, 0), (0, 2, 1), (0, 1, 1), (0, 3, 1)]
LATE = [(1, 1, 1), (1, 2, 1), (1, 3, 1), (1, 0, 1)]
CHIPS = [(1, 2), (0, 2), (1, 1), (1, 3), (1, 0), (0, 1), (0, 3)]
OTHERS = [(1, 2), (0, 2), (1, 1), (1, 3), (1, 0), (0, 1), (0, 3)]
CHUNKS = 4


def turn(o, c):
    return o[1] + 2 * c if o[0] else o[1]


def source(o):
    xh, z, c = (lax.axis_index(a) for a in COL)
    xh, c = lax.rem(xh + 2 - o[0], 2), lax.rem(c + 2 - o[2], 2)
    return xh * 8 + lax.rem(z + 8 - turn(o, c), 4) * 2 + c


def update(k, out, summed, rs, read):
    def tile(t, _):
        at = pl.multiple_of(k * BLK + t * 128, 128)
        scale = jnp.broadcast_to(rs[pl.ds(k * 32 + t, 1), :], (16, 128))
        out[0, :, pl.ds(at, 128)] = read(at, t) - summed[:, pl.ds(at, 128)] * scale
        return 0
    lax.fori_loop(0, 32, tile, 0, unroll=8)


def kernel(tab, st, slot_h, ids_h, grads, out, state_out, summed, rs, slot, ids_all, tabv, tT, gv, rA, sB, rB,
           ids_t, hot, hot1, same, acc, X, stf, qs, qp, qh, rq, tot, seml, ssem, rsem, sst, rst, sq, rq_sem,
           sA, rsA, sBs, rsB):
    xl, y, xh, z, c = (lax.axis_index(a) for a in SRC + COL)
    src = xl * 4 + y
    col = xh * 8 + z * 2 + c

    def remote(a, b, sems, i, device):
        cp = pltpu.make_async_remote_copy(
            src_ref=a, dst_ref=b, send_sem=sems[0].at[i], recv_sem=sems[1].at[i],
            device_id=device, device_id_type=MESH)
        cp.start()
        return cp

    def peer(o):
        return (xl, y, lax.rem(xh + o[0], 2), lax.rem(z + o[1], 4), lax.rem(c + o[2], 2))

    def other(o):
        nxl, ny = lax.rem(xl + o[0], 2), lax.rem(y + o[1], 4)
        return (nxl, ny, xh, z, c), nxl * 4 + ny

    partner = peer((0, 0, 1))

    barrier = pltpu.get_barrier_semaphore()
    for o in PEERS:
        pl.semaphore_signal(barrier, inc=1, device_id=peer(o), device_id_type=MESH)
    for o in OTHERS:
        pl.semaphore_signal(barrier, inc=1, device_id=other(o)[0], device_id_type=MESH)

    rows = BLK // CHUNKS
    first = pl.multiple_of((1 - xh) * 128, 128)
    second = pl.multiple_of(xh * 128, 128)
    small = []
    for i, (a, b) in enumerate([(grads.at[0], gv), (slot_h, slot), (ids_h, ids_all), (st, stf.at[xh, z, c])]):
        cp = pltpu.make_async_copy(a, b, seml.at[i])
        cp.start()
        small.append(cp)
    loads = []
    for h, lanes in enumerate((first, second)):
        for i in range(CHUNKS):
            cp = pltpu.make_async_copy(
                tab.at[0, pl.ds(i * rows, rows), pl.ds(lanes, 128)], tabv.at[h, pl.ds(i * rows, rows)],
                seml.at[4 + h * CHUNKS + i])
            cp.start()
            loads.append(cp)

    def columns(h, chunks=range(CHUNKS)):
        for i in chunks:
            loads[h * CHUNKS + i].wait()
            part = tabv[h, pl.ds(i * rows, rows), :]
            tT[h, :, :, pl.ds(i * rows, rows)] = part.T.reshape(8, 16, rows)

    sends_t = {}

    def send_tables(group):
        for o in group:
            nz, nc = lax.rem(z + turn(o, c), 4), lax.rem(c + o[2], 2)
            sends_t[o] = remote(
                tT.at[1 - o[0], nz * 2 + nc], out.at[0, :, pl.ds(pl.multiple_of(col * BLK, BLK), BLK)],
                (ssem, rsem), PEERS.index(o), (xl, y, lax.rem(xh + o[0], 2), nz, nc))

    columns(0, range(CHUNKS // 2))
    for cp in small:
        cp.wait()
    pl.semaphore_wait(barrier, len(PEERS) + len(OTHERS))

    sends_a = []
    for i, o in enumerate(OTHERS):
        device, k = other(o)
        sends_a.append(remote(gv.at[:, pl.ds(pl.multiple_of(k * 256, 256), 256)], rA.at[src], (sA, rsA), i, device))
    columns(0, range(CHUNKS // 2, CHUNKS))
    state_x = remote(stf.at[xh, z, c], stf.at[xh, z, c], (sst, rst), 0, peer((1, 0, 0)))
    send_tables(FIRST_X)
    columns(1)
    send_tables(FIRST_Z)
    rA[src] = gv[:, pl.ds(pl.multiple_of(src * 256, 256), 256)]

    ids = ids_all[pl.ds(slot[src], 1), :]
    for i in range(16):
        tile = jnp.broadcast_to(ids[:, i * 128:(i + 1) * 128], (128, 128))
        ids_t[pl.ds(i * 128, 128), :] = tile.T

    for cp in sends_a:
        cp.wait_recv()
    for i, o in enumerate(OTHERS):
        sB[i] = rA[slot[other(o)[1]]]
    rB[src] = rA[slot[src]]
    state_x.wait_recv()
    state_z = [remote(stf.at[:, z, c], stf.at[:, z, c], (sst, rst), i, peer((0, i, 0))) for i in (1, 2, 3)]
    sends_b = []
    for i, o in enumerate(OTHERS):
        sends_b.append(remote(sB.at[i], rB.at[src], (sBs, rsB), i, other(o)[0]))
    send_tables(SECOND)

    lane = lax.broadcasted_iota(jnp.int32, (256, 128), 1)
    for i in range(8):
        at = jnp.bitwise_and(ids_t[pl.ds(i * 256, 256), :], 255)
        low = (at == lane).astype(f32)
        high = (at == lane + 128).astype(f32)
        hot[pl.ds(i * 256, 256), pl.ds(0, 128)] = low.astype(bf16)
        hot[pl.ds(i * 256, 256), pl.ds(128, 128)] = high.astype(bf16)
        hot1[pl.ds(i * 256, 256), :] = (low + high).astype(bf16)
    for i in range(8):
        row = ids_t[pl.ds(i * 256, 256), :]
        for k in range(16):
            same[pl.ds(i * 256, 256), pl.ds(k * 128, 128)] = (
                row == ids[:, k * 128:(k + 1) * 128]).astype(f32).astype(bf16)

    def parts(v):
        a = v.astype(bf16)
        v = v - a.astype(f32)
        b = v.astype(bf16)
        v = v - b.astype(f32)
        return a, b, v.astype(bf16)

    for cp in sends_b:
        cp.wait_recv()
    g = [parts(rB[p]) for p in range(8)]
    g = [jnp.concatenate([g[p][k] for p in range(8)], axis=1) for k in range(3)]
    lhs = jnp.concatenate(g + [jnp.ones((16, UPD), bf16)], axis=0)

    for i in range(8):
        part = jnp.dot(lhs[:, i * 256:(i + 1) * 256], same[pl.ds(i * 256, 256), :], preferred_element_type=f32)
        if i == 0:
            acc[...] = part
        else:
            acc[...] += part
    s = acc[0:16, :] + acc[16:32, :] + acc[32:48, :]
    q = jnp.sum(s * s, axis=0, keepdims=True)
    qs[0] = q[:, :1024]
    qs[1] = q[:, 1024:]

    high = jnp.broadcast_to(lax.shift_right_logical(ids, 8).astype(f32).astype(bf16), (16, UPD))
    zero = jnp.zeros((16, UPD), bf16)

    def dense(it, _):
        for r in range(16):
            want = (it * 16 + r).astype(f32).astype(bf16)
            mask = high == want
            for k in range(3):
                X[pl.ds(k * 256 + r * 16, 16), :] = jnp.where(mask, g[k], zero)
        o = jnp.dot(X[...], hot[...], preferred_element_type=f32)
        o = o[0:256] + o[256:512] + o[512:768]
        for r in range(16):
            summed[:, pl.ds(pl.multiple_of((it * 16 + r) * 256, 256), 256)] = o[r * 16:(r + 1) * 16]
        return 0

    q_core = remote(qs.at[1 - c], qp, (sq, rq_sem), 7, partner)
    lax.fori_loop(0, 1, dense, 0)
    q_core.wait()
    half = qs[c] + qp[...]
    qh[...] = half
    rq[xh * 4 + z] = half
    sends_q = [remote(qh, rq.at[xh * 4 + z], (sq, rq_sem), i, peer((*o, 0))) for i, o in enumerate(CHIPS)]
    send_tables(THIRD)
    lax.fori_loop(1, 14, dense, 0)
    for cp in state_z:
        cp.wait_recv()
    state_c = remote(stf.at[:, :, c], stf.at[:, :, c], (sst, rst), 4, partner)
    for cp in sends_q:
        cp.wait_recv()
    total = rq[0]
    for k in range(1, 8):
        total = total + rq[k]
    tot[c] = total
    lax.fori_loop(14, 15, dense, 0)
    q_back = remote(tot.at[c], tot.at[c], (sq, rq_sem), 8, partner)
    lax.fori_loop(15, 16, dense, 0)
    q_back.wait_recv()
    state_c.wait_recv()

    total = jnp.concatenate([tot[0], tot[1]], axis=1) / acc[48:49, :]
    tp = [jnp.broadcast_to(t, (16, UPD)) for t in parts(total)]
    low = lax.shift_right_logical(ids, 7)
    for b in range(4):
        for r in range(8):
            row = lax.broadcasted_iota(jnp.int32, (16, UPD), 0) + (b * 128 + r * 16)
            mask = (row == jnp.broadcast_to(low, (16, UPD))).astype(f32).astype(bf16)
            for k in range(3):
                X[pl.ds(k * 128 + r * 16, 16), :] = mask * tp[k]
        o = jnp.dot(X[pl.ds(0, 384), :], hot1[...], preferred_element_type=f32)
        saved = stf[b // 2, (b % 2) * 2:(b % 2) * 2 + 2].reshape(128, 128)
        new = saved + (o[0:128] + o[128:256] + o[256:384]) / D
        state_out[pl.ds(b * 128, 128), :] = new
        rs[pl.ds(b * 128, 128), :] = learn_rate / (jnp.sqrt(new) + epsilon)

    update(col, out, summed, rs, lambda at, t: tT[1, z * 2 + c, :, pl.ds(pl.multiple_of(t * 128, 128), 128)])
    for o in EARLY:
        sends_t[o].wait_recv()
        update(source(o), out, summed, rs, lambda at, t: out[0, :, pl.ds(at, 128)])
    for o in LATE:
        sends_t[o].wait_recv()
    for cp in sends_a + sends_b + state_z + sends_q + [state_x, state_c, q_back]:
        cp.wait_send()
    for o in PEERS:
        sends_t[o].wait_send()


def finish(landed, state, summed, rs, out, state_out, sem):
    col = source((0, 0, 0))
    copies = [pltpu.make_async_copy(state, state_out, sem.at[16])]
    copies[0].start()

    def put(k):
        at = pl.ds(pl.multiple_of(k * BLK, BLK), BLK)
        cp = pltpu.make_async_copy(landed.at[0, :, at], out.at[0, :, at], sem.at[len(copies) - 1])
        cp.start()
        copies.append(cp)

    put(col)
    for o in EARLY:
        put(source(o))
    for o in LATE:
        update(source(o), landed, summed, rs, lambda at, t: landed[0, :, pl.ds(at, 128)])
        put(source(o))
    for cp in copies:
        cp.wait()


def body(saved_tables, saved_state, slot_table, row_ids, grads):
    n, m = len(PEERS), len(OTHERS)
    dma = pltpu.SemaphoreType.DMA
    vmem = pl.BlockSpec(memory_space=pltpu.VMEM)
    hbm = pl.BlockSpec(memory_space=pltpu.HBM)
    tables, state, summed, rs = pl.pallas_call(
        kernel,
        out_shape=(pltpu.VMEM((1, 16, ROWS), f32), pltpu.VMEM((512, 128), f32), pltpu.VMEM((16, ROWS), f32),
                   pltpu.VMEM((512, 128), f32)),
        in_specs=[hbm] * 5,
        out_specs=(vmem,) * 4,
        scratch_shapes=[
            pltpu.SMEM((8,), jnp.int32), pltpu.VMEM((8, UPD), jnp.int32),
            pltpu.VMEM((2, BLK, 128), f32), pltpu.VMEM((2, 8, 16, BLK), f32), pltpu.VMEM((16, UPD), f32),
            pltpu.VMEM((8, 16, 256), f32), pltpu.VMEM((7, 16, 256), f32), pltpu.VMEM((8, 16, 256), f32),
            pltpu.VMEM((UPD, 128), jnp.int32), pltpu.VMEM((UPD, 256), bf16), pltpu.VMEM((UPD, 128), bf16),
            pltpu.VMEM((UPD, UPD), bf16), pltpu.VMEM((64, UPD), f32), pltpu.VMEM((768, UPD), bf16),
            pltpu.VMEM((2, 4, 2, 32, 128), f32), pltpu.VMEM((2, 1, 1024), f32), pltpu.VMEM((1, 1024), f32),
            pltpu.VMEM((1, 1024), f32), pltpu.VMEM((8, 1, 1024), f32), pltpu.VMEM((2, 1, 1024), f32),
            dma((4 + 2 * CHUNKS,)), dma((n,)), dma((n,)), dma((5,)), dma((5,)),
            dma((9,)), dma((9,)), dma((m,)), dma((m,)), dma((m,)), dma((m,)),
        ],
        compiler_params=pltpu.CompilerParams(
            collective_id=0, has_side_effects=True, vmem_limit_bytes=44 << 20),
        name="restore",
    )(*(pltpu.with_memory_space_constraint(a, pltpu.HBM) for a in (
        saved_tables, saved_state.reshape(32, 128), slot_table, row_ids, grads)))
    tables, state = pl.pallas_call(
        finish,
        out_shape=(jax.ShapeDtypeStruct((1, 16, ROWS), f32), jax.ShapeDtypeStruct((512, 128), f32)),
        in_specs=[vmem] * 4,
        out_specs=(hbm, hbm),
        scratch_shapes=[dma((17,))],
        compiler_params=pltpu.CompilerParams(vmem_limit_bytes=16 << 20),
        name="finish",
    )(tables, state, summed, rs)
    return (tables, state.reshape(1, ROWS))


def solution(mesh):
    split = Mesh(mesh.devices.reshape(2, 4, 2, 4, 2), SRC + COL)
    in_specs = (P(SRC, COL, None), P(SRC, COL), P(), P(), P(SRC, COL, None))
    out_specs = (P(SRC, COL, None), P(SRC, None))
    return jax.shard_map(body, mesh=split, in_specs=in_specs, out_specs=out_specs, check_vma=False)
```
